32 devices in a mesh: region: 2 (over core), cells: 16 (over z, y, x).
Axes of the slice: x: 2, y: 2, z: 4, core: 2. Of those that a mesh axis runs over, the one named last changes fastest.
Arguments:
- moments: float32 [2, 6, 4, 128, 2048], P('region', None, None, None, 'cells'), may hold values from 0 to 40, as said below
- courant_azimuth: float32 [2, 4, 128, 2048], P('region', None, None, 'cells'), may hold values from 0.1 to 0.3
- courant_radial: float32 [2, 4, 128, 2048], P('region', None, None, 'cells'), may hold values from -0.25 to 0.25
- courant_axial: float32 [2, 4, 128, 2048], P('region', None, None, 'cells'), may hold values from -0.2 to 0.2
- shear: float32 [2, 4, 128, 2048], P('region', None, None, 'cells'), may hold values from 0.5 to 4
- owner: int32 [2, 2048, 1], P('region', 'cells'), may hold values from 0 to 15; in each aligned block of 128 rows (0 to 127, 128 to 255, ..., all dimensions but the last counted through in order) at most 16 rows name the same one
- target: int32 [2, 2048], P('region', 'cells'), may hold values from 0 to 127
- ami_weight: float32 [2, 2048, 128, 128], P('region', 'cells'), may hold values from 0 to 1, as said below
Outputs:
- updated: float32 [2, 6, 4, 128, 2048], P('region', None, None, None, 'cells')
The draws below stay inside these ranges and needn't reach their ends.
Inputs may be any that keep to these rules, and one draw needn't show every extreme that they name: The rows of one device name each owner at most 16 times. Each cell's six entries are the moments of orders 0 to 5 of a positive measure on three or more sizes between 0.3 and 1.6. `ami_weight`: all entries are nonnegative.
All inputs are finite; a program needn't handle non-finite values.
Results may differ from the reference program's by a relative error of at most 0.0003.
Values sent between devices are 32-bit elements; how exact they have to be, the bound alone decides.
No kernel may reach another device: no remote copies, remote signals or barrier semaphores. Data moves between devices by JAX's collectives and lax.ppermute only.
A program may use at most 64 MiB of HBM per device.

```python
import math
import jax
import jax.numpy as jnp
import numpy as np
from jax import lax

LAYERS = 4
ROWS = 128
FACES = 128
CAP = 16
AZIMUTH = 2048
BLOCKS = 2048
N_CELLS = 16


def draw_moments(key, part):
    shape = (2, LAYERS, ROWS, AZIMUTH)
    subkeys = jax.random.split(jax.random.fold_in(key, 11), 6)
    lower = (0.3, 0.7, 1.1)
    upper = (0.6, 1.0, 1.5)
    weight_lo = 0.01
    weight_hi = 1.2
    nodes = jnp.stack([jax.random.uniform(subkeys[index], shape, jnp.float32, lower[index], upper[index]) for index in range(3)])
    logs = jnp.stack([jax.random.uniform(subkeys[3 + index], shape, jnp.float32, jnp.log(weight_lo), jnp.log(weight_hi)) for index in range(3)])
    weights = jnp.exp(logs)
    return jnp.stack([jnp.sum(weights * nodes ** degree, axis=0) for degree in range(6)], axis=1)


def draw_courant_radial(key, part):
    shape = (2, LAYERS, ROWS, AZIMUTH)
    subkeys = jax.random.split(jax.random.fold_in(key, 37), 2)
    interior = jax.random.uniform(subkeys[0], shape, jnp.float32, -0.25, 0.25)
    magnitude = jax.random.uniform(subkeys[1], shape, jnp.float32, 0.15, 0.25)
    region_idx = jnp.arange(2)[:, None, None, None]
    layer_idx = jnp.arange(LAYERS)[None, :, None, None]
    rotor_edge = jnp.logical_and(region_idx == 0, layer_idx == LAYERS - 1)
    stator_edge = jnp.logical_and(region_idx == 1, layer_idx == 0)
    field = jnp.where(rotor_edge, -magnitude, interior)
    return jnp.where(stator_edge, magnitude, field)


def draw_ami_weight(key, part):
    subkeys = jax.random.split(jax.random.fold_in(key, 23), 2)
    diagonal = jax.random.uniform(subkeys[0], (2, BLOCKS, FACES), jnp.float32, 0.3, 0.7)
    spread = 0.5 / FACES
    offdiag = jax.random.uniform(subkeys[1], (2, BLOCKS, FACES, FACES), jnp.float32, 0.0, 1.0) * spread
    return offdiag + diagonal[..., None] * jnp.eye(FACES, dtype=jnp.float32)


def plant(entries, rng, smallest, high):
    longest = entries.shape.index(max(entries.shape))
    spots = []
    for shift in (0, 1):
        where = [jax.random.randint(jax.random.fold_in(rng, axis), (), 0, length) for axis, length in enumerate(entries.shape)]
        where[longest] = (where[longest] + shift) % entries.shape[longest]
        spots.append(tuple(where))
    return entries.at[spots[0]].set(smallest).at[spots[1]].set(high)


def level_of(key, shape, pieces, low, high):
    gain, own = 1.0, jax.random.fold_in(key, 6)
    for position, parts in pieces:
        heights = jnp.exp(jax.random.uniform(jax.random.fold_in(own, position), (parts,), jnp.float32, low / len(pieces), high / len(pieces)))
        gain = gain * jnp.repeat(heights, shape[position] // parts).reshape([-1 if axis == position else 1 for axis in range(len(shape))])
    return gain


def shared_out(stream_key, own, number, rows, number_of, top, limit, lean):
    ranking = jax.random.permutation(stream_key, number_of)
    heavy_load, common = shares(number_of, rows * top, limit, lean, True), shares(number_of, rows * top, limit, lean, False)
    places = jnp.arange(number_of)

    def named(tallies, turn):
        used = int((tallies > 0).sum())
        fixed = max(1, used // 4)
        passed = fixed + (places - fixed + turn * (used - fixed)) % max(1, number_of - fixed)
        return jnp.zeros((number_of,), jnp.int32).at[ranking[jnp.where(places < fixed, places, passed)]].set(jnp.asarray(tallies, jnp.int32))

    tallies = jnp.where(number % 4 == 0, named(heavy_load, number // 4), named(common, number - number // 4 - 1))
    mixed = jax.random.permutation(jax.random.fold_in(own, 3), number_of)
    donor, taker = mixed[0:number_of // 2 * 2:2], mixed[1:number_of // 2 * 2:2]
    slack = jnp.minimum(tallies[donor] - 1, limit - tallies[taker]) // 2
    slack = jnp.where((donor == ranking[0]) | (taker == ranking[0]) | (tallies[taker] == 0), 0, jnp.maximum(slack, 0))
    passed = jax.random.randint(jax.random.fold_in(own, 4), (number_of // 2,), 0, 1 << 20) % (slack + 1)
    tallies = tallies.at[donor].add(-passed).at[taker].add(passed)
    members = jnp.searchsorted(jnp.cumsum(tallies), jnp.arange(rows * top), side="right").astype(jnp.int32)
    grid = members.reshape(top, rows).T
    grid = grid[jax.random.permutation(jax.random.fold_in(own, 1), rows)]
    turn = jax.random.randint(jax.random.fold_in(own, 2), (rows, 1), 0, top)
    return jnp.take_along_axis(grid, (jnp.arange(top)[None, :] + turn) % top, axis=1)


def shares(number_of, total, most, slope, full):
    portions = [(1 << 20) // math.isqrt(rank ** slope) + 1 for rank in range(1, number_of + 1)]
    largest = most if full else min(most, max(-(-total // number_of), total * portions[0] // sum(portions)))
    least = 1 if total - largest >= number_of - 1 else 0
    counts, rest = [largest] + [least] * (number_of - 1), total - largest - least * (number_of - 1)
    while rest > 0:
        movable = [i for i in range(1, number_of) if counts[i] < largest] or [i for i in range(1, number_of) if counts[i] < most]
        whole, left = sum([portions[i] for i in movable]), rest
        for i in movable:
            extra = min(most - counts[i], max(1, left * portions[i] // whole), rest)
            counts[i] = counts[i] + extra
            rest = rest - extra
    return np.array(counts)


def setup_inputs(seed: int = 0) -> dict:
    keys = jax.random.split(jax.random.key(seed), 9)
    moments = draw_moments(jax.random.fold_in(keys[8], 71), 0)
    courant_azimuth = jnp.clip(0.1 + 0.20000001043081284 * jax.random.uniform(keys[1], (2, LAYERS, ROWS, AZIMUTH), jnp.float32) ** level_of(keys[1], (2, LAYERS, ROWS, AZIMUTH), ((0, 2), (3, 16)), -0.2, 0.2), 0.1, 0.3)
    courant_radial = draw_courant_radial(jax.random.fold_in(keys[8], 71), 0)
    courant_axial = jnp.clip(jax.random.uniform(keys[3], (2, LAYERS, ROWS, AZIMUTH), jnp.float32, -0.2, 0.2) * level_of(keys[3], (2, LAYERS, ROWS, AZIMUTH), ((0, 2), (3, 16)), -0.4, 0.0), -0.2, 0.2)
    shear = jnp.clip(jnp.exp(math.log(4.0) - 2.0794415 * jax.random.uniform(keys[4], (2, LAYERS, ROWS, AZIMUTH), jnp.float32) ** level_of(keys[4], (2, LAYERS, ROWS, AZIMUTH), ((0, 2), (3, 16)), -0.2, 0.2)), 0.5, 4.0)
    owner_keys = jax.random.split(jax.random.fold_in(keys[5], 1), 2 * BLOCKS // ROWS)
    owner_turns = jax.random.permutation(jax.random.fold_in(keys[5], 3), 2 * BLOCKS // ROWS)
    owner = jax.vmap(lambda own, number: shared_out(jax.random.fold_in(keys[5], 2), own, number, ROWS, N_CELLS, 1, CAP, 2))(owner_keys, owner_turns).reshape((2, BLOCKS, 1))
    target = plant(jax.random.randint(keys[6], (2, BLOCKS), 0, ROWS), jax.random.fold_in(keys[6], 1), 0, ROWS - 1).astype(jnp.int32)
    ami_weight = draw_ami_weight(jax.random.fold_in(keys[8], 71), 0)
    return {"moments": moments, "courant_azimuth": courant_azimuth, "courant_radial": courant_radial, "courant_axial": courant_axial, "shear": shear, "owner": owner, "target": target, "ami_weight": ami_weight}


KAGG = 0.005
KBRK = 0.02

def quadrature(moment):
    mass = moment[0]
    scaled = [moment[degree] / mass for degree in range(6)]
    mean_size = scaled[1]
    first_two = scaled[2] - mean_size * scaled[1]
    first_three = scaled[3] - mean_size * scaled[2]
    first_four = scaled[4] - mean_size * scaled[3]
    first_five = scaled[5] - mean_size * scaled[4]
    alpha_one = first_three / first_two - mean_size
    beta_one = first_two
    second_two = first_four - alpha_one * first_three - beta_one * scaled[2]
    second_three = first_five - alpha_one * first_four - beta_one * scaled[3]
    alpha_two = second_three / second_two - first_three / first_two
    beta_two = second_two / first_two
    centre = (mean_size + alpha_one + alpha_two) / 3.0
    dev_zero = mean_size - centre
    dev_one = alpha_one - centre
    dev_two = alpha_two - centre
    spread = jnp.sqrt((dev_zero * dev_zero + dev_one * dev_one + dev_two * dev_two + 2.0 * (beta_one + beta_two)) / 6.0)
    determ = dev_zero * (dev_one * dev_two - beta_two) - beta_one * dev_two
    cosine = jnp.clip(determ / (2.0 * spread * spread * spread), -1.0, 1.0)
    third = jnp.arccos(cosine) / 3.0
    node_high = centre + 2.0 * spread * jnp.cos(third)
    node_low = centre + 2.0 * spread * jnp.cos(third + 2.0 * math.pi / 3.0)
    node_mid = 3.0 * centre - node_high - node_low
    nodes = [node_low, node_mid, node_high]
    weights = []
    for node in nodes:
        lead = node - mean_size
        trail = (node - alpha_one) * lead - beta_one
        norm_sq = 1.0 + lead * lead / beta_one + trail * trail / (beta_one * beta_two)
        weights.append(mass / norm_sq)
    return (nodes, weights)

def sources(moment, shear):
    nodes, weights = quadrature(moment)
    cubes = [node * node * node for node in nodes]
    pairs = []
    for first in range(3):
        for second in range(3):
            summed = nodes[first] + nodes[second]
            kernel = shear * summed * summed * summed
            pairs.append((first, second, weights[first] * weights[second] * kernel, jnp.log(cubes[first] + cubes[second])))
    result = []
    for degree in range(6):
        birth = jnp.zeros_like(shear)
        death = jnp.zeros_like(shear)
        for first, second, pair, logsum in pairs:
            birth = birth + 0.5 * pair * jnp.exp(degree / 3.0 * logsum)
            death = death + pair * nodes[first] ** degree
        factor = 2.0 ** (1.0 - degree / 3.0) - 1.0
        breakage = jnp.zeros_like(shear)
        for index in range(3):
            breakage = breakage + weights[index] * KBRK * shear * cubes[index] * factor * nodes[index] ** degree
        result.append(moment[degree] + KAGG * (birth - death) + breakage)
    return jnp.stack(result)

def advance(moment, previous, ghost_layer, is_rotor, azim, radial, axial, shear):
    empty_layer = jnp.zeros_like(ghost_layer)
    beyond_edge = jnp.where(is_rotor, ghost_layer, empty_layer)
    below_edge = jnp.where(is_rotor, empty_layer, ghost_layer)
    prev_azim = jnp.concatenate([previous[..., None], moment[..., :-1]], axis=3)
    radial_below = jnp.concatenate([below_edge[:, None], moment[:, :-1]], axis=1)
    radial_beyond = jnp.concatenate([moment[:, 1:], beyond_edge[:, None]], axis=1)
    axial_pad = jnp.zeros_like(moment[:, :, :1])
    axial_below = jnp.concatenate([axial_pad, moment[:, :, :-1]], axis=2)
    axial_beyond = jnp.concatenate([moment[:, :, 1:], axial_pad], axis=2)
    advected = moment - azim * (moment - prev_azim) - jnp.maximum(radial, 0.0) * (moment - radial_below) - jnp.minimum(radial, 0.0) * (radial_beyond - moment) - jnp.maximum(axial, 0.0) * (moment - axial_below) - jnp.minimum(axial, 0.0) * (axial_beyond - moment)
    return sources([advected[degree] for degree in range(6)], shear)

def reference(moments, courant_azimuth, courant_radial, courant_axial, shear, owner, target, ami_weight):
    groups = 2 * N_CELLS
    blocked = moments.reshape(2, 6, LAYERS, ROWS, N_CELLS, FACES).transpose(0, 4, 1, 2, 3, 5).reshape(groups, 6, LAYERS, ROWS, FACES)

    def split_field(field):
        return field.reshape(2, LAYERS, ROWS, N_CELLS, FACES).transpose(0, 3, 1, 2, 4).reshape(groups, LAYERS, ROWS, FACES)
    azim_b = split_field(courant_azimuth)
    radial_b = split_field(courant_radial)
    axial_b = split_field(courant_axial)
    shear_b = split_field(shear)
    rotor_flags = jnp.arange(groups) < N_CELLS
    layers = jnp.where(rotor_flags[:, None, None, None], blocked[:, :, LAYERS - 1], blocked[:, :, 0])
    weights_b = ami_weight.reshape(groups, ROWS, FACES, FACES)

    def weigh(pair):
        return jnp.einsum('zfg,kzg->zkf', pair[0], pair[1], precision=lax.Precision.HIGHEST)
    contrib = lax.map(weigh, (weights_b, layers)).reshape(2, N_CELLS * ROWS, 6, FACES)
    dest = owner[:, :, 0] * ROWS + target
    empty = jnp.zeros((N_CELLS * ROWS, 6, FACES), jnp.float32)
    ghost_rotor = empty.at[dest[1]].add(contrib[1])
    ghost_stator = empty.at[dest[0]].add(contrib[0])
    ghost = jnp.stack([ghost_rotor, ghost_stator]).reshape(2, N_CELLS, ROWS, 6, FACES).transpose(0, 1, 3, 2, 4).reshape(groups, 6, ROWS, FACES)
    rims = blocked[..., FACES - 1].reshape(2, N_CELLS, 6, LAYERS, ROWS)
    rims = jnp.roll(rims, 1, axis=1).reshape(groups, 6, LAYERS, ROWS)

    def step_block(items):
        return advance(items[0], items[1], items[2], items[3], items[4], items[5], items[6], items[7])
    updated = lax.map(step_block, (blocked, rims, ghost, rotor_flags, azim_b, radial_b, axial_b, shear_b))
    return updated.reshape(2, N_CELLS, 6, LAYERS, ROWS, FACES).transpose(0, 2, 3, 4, 1, 5).reshape(2, 6, LAYERS, ROWS, N_CELLS * FACES)
```

```python
import functools
import math

import jax
import jax.numpy as jnp
from jax import lax
from jax.experimental import pallas as pl
from jax.experimental.pallas import tpu as pltpu
from jax.sharding import PartitionSpec as P


KAGG = 0.005
KBRK = 0.02
ORDERS = 6
F32 = jnp.float32
BF16 = jnp.bfloat16
KERNEL_VMEM = 8 * 1024 * 1024
PAD = 8
GROUP = 8
TILE = 32
FULL_VMEM = 58 * 1024 * 1024
BOUNDS = (0, 4, 8, 12, 14, 16)
IN_VMEM = pl.BlockSpec(memory_space=pltpu.VMEM)
IN_HBM = pl.BlockSpec(memory_space=pltpu.HBM)

COS_THIRD = (
    0.44444444535893496,
    0.04115211563399856,
    0.009758495429256357,
    0.0029417445898478234,
    0.0012216398155368902,
    -0.00013418618671007774,
    0.0009423656998505278,
    -0.000598812660480466,
    0.00027219066323123,
)


def two_parts(value):
    high = value.astype(BF16)
    return high, (value - high.astype(F32)).astype(BF16)


def quadrature(moment):
    inv_mass = 1.0 / moment[0]
    n1, n2, n3, n4, n5 = [moment[degree] * inv_mass for degree in range(1, 6)]
    p1 = n2 - n1 * n1
    p2 = n3 - n1 * n2
    p3 = n4 - n1 * n3
    p4 = n5 - n1 * n4
    inv_p1 = 1.0 / p1
    slope = p2 * inv_p1
    a1 = slope - n1
    q2 = p3 - a1 * p2 - p1 * n2
    q3 = p4 - a1 * p3 - p1 * n3
    inv_q2 = 1.0 / q2
    a2 = q3 * inv_q2 - slope
    b2 = q2 * inv_p1
    centre = (n1 + a1 + a2) * (1.0 / 3.0)
    d0 = n1 - centre
    d1 = a1 - centre
    d2 = a2 - centre
    square = (d0 * d0 + d1 * d1 + d2 * d2 + 2.0 * (p1 + b2)) * (1.0 / 6.0)
    inv_h = lax.rsqrt(square)
    h = square * inv_h
    determ = d0 * (d1 * d2 - b2) - p1 * d2
    cosine = jnp.clip(determ * 0.5 * (inv_h * inv_h * inv_h), -1.0, 1.0)
    half = jnp.sqrt(0.5 + 0.5 * cosine)
    w = (0.5 - 0.5 * cosine) / (1.0 + half)
    q = jnp.full_like(w, COS_THIRD[-1])
    for term in COS_THIRD[-2::-1]:
        q = q * w + term
    drop = w * q
    h_cos = h * (1.0 - drop)
    h_sin = h * jnp.sqrt(drop * (2.0 - drop)) * math.sqrt(3.0)
    high = centre + 2.0 * h_cos
    low = centre - h_cos - h_sin
    mid = 3.0 * centre - high - low
    nodes = (low, mid, high)
    weights = []
    for node in nodes:
        u = node - n1
        v = (node - a1) * u - p1
        weights.append(moment[0] / (1.0 + u * u * inv_p1 + v * v * inv_q2))
    return nodes, weights


def sources(moment, shear):
    nodes, weights = quadrature(moment)
    cubes = [node * node * node for node in nodes]
    rate = KBRK * shear
    agg = KAGG * shear
    breaks = [weights[i] * rate * cubes[i] for i in range(3)]
    equal = [weights[i] * agg * (4.0 * cubes[i]) * weights[i] for i in range(3)]
    lost = [2.0 * equal[i] for i in range(3)]
    pairs = []
    for i, j in ((0, 1), (0, 2), (1, 2)):
        summed = nodes[i] + nodes[j]
        pair = weights[i] * weights[j] * (agg * summed * summed * summed)
        lost[i] = lost[i] + pair
        lost[j] = lost[j] + pair
        volume = cubes[i] + cubes[j]
        root = jnp.exp(jnp.log(volume) * (1.0 / 3.0))
        pairs.append((pair, root, volume))
    updated = []
    node_powers = [jnp.ones_like(shear)] * 3
    for degree in range(ORDERS):
        grow = 2.0 ** (degree / 3.0)
        split = 2.0 ** (1.0 - degree / 3.0) - 1.0
        total = moment[degree]
        for i in range(3):
            net = grow * equal[i] - lost[i]
            if degree != 3:
                net = net + split * breaks[i]
            if degree > 0:
                net = net * node_powers[i]
            total = total + net
        for pair, root, volume in pairs:
            factor = (None, root, root * root, volume, volume * root, volume * root * root)[degree]
            total = total + (pair if factor is None else pair * factor)
        updated.append(total)
        node_powers = [power * node for power, node in zip(node_powers, nodes)] if degree else list(nodes)
    return updated


def dispatch_body(
    cap, owner_hbm, target_hbm, moments_hbm, weight_hbm, out, rim,
    moments, weight, source, ids, owner, target, count, index_sem, moment_sem, weight_sem,
):
    layers, rows, faces = moments.shape[1:]
    peers = count.shape[0]
    block = ORDERS * cap + 1
    rotor = lax.axis_index("region") == 0
    layer = jnp.where(rotor, layers - 1, 0)

    def layer_copy(index):
        which = jnp.where(rotor, layers - 1 - index, index)
        return pltpu.make_async_copy(moments_hbm.at[:, which], moments.at[:, which], moment_sem.at[index])

    def weight_copy(step):
        part = pl.ds(BOUNDS[step] * rows // BOUNDS[-1], (BOUNDS[step + 1] - BOUNDS[step]) * rows // BOUNDS[-1])
        return pltpu.make_async_copy(weight_hbm.at[part], weight.at[part], weight_sem.at[step])

    index_copies = (
        pltpu.make_async_copy(owner_hbm, owner, index_sem.at[0]),
        pltpu.make_async_copy(target_hbm, target, index_sem.at[1]),
    )
    layer_copy(0).start()
    for copy in index_copies:
        copy.start()
    for step in range(len(BOUNDS) - 1):
        weight_copy(step).start()
        if step == 0:
            for index in range(1, layers):
                layer_copy(index).start()

    out[...] = jnp.zeros_like(out)
    lane = lax.broadcasted_iota(jnp.int32, (1, faces), 1)
    offset = (lax.axis_index("cells") * cap) % faces
    mine = jnp.logical_and(lane >= offset, lane < offset + cap)
    ids[...] = jnp.broadcast_to(jnp.where(mine, -1.0, 0.0), ids.shape)

    @pl.loop(0, peers)
    def _(peer):
        count[peer] = 0

    source[pl.ds(ORDERS * rows, (PAD - ORDERS) * rows)] = jnp.zeros(((PAD - ORDERS) * rows, faces), F32)
    layer_copy(0).wait()
    for degree in range(ORDERS):
        source[pl.ds(degree * rows, rows)] = moments[degree, layer]
    for copy in index_copies:
        copy.wait()
    width = PAD * GROUP
    column = (lax.broadcasted_iota(jnp.int32, (faces, 2 * width), 1) % width) // PAD
    turned = []
    for first in range(0, rows, GROUP):
        value = jnp.concatenate([source[pl.ds(first + i, PAD, stride=rows)] for i in range(GROUP)], axis=0)
        high = value.astype(BF16).astype(F32)
        turned.append(jnp.concatenate([high, value - high], axis=0).T)

    def place(first, product):
        product = product.T
        product = product[:width] + product[width:]
        for i in range(GROUP):
            peer = owner[first + i]
            rank = count[peer]
            count[peer] = rank + 1
            out[pl.ds(peer * block + rank * ORDERS, ORDERS), :] = product[PAD * i : PAD * i + ORDERS]
            ids[pl.ds(peer, 1), :] = jnp.where(
                lane == offset + rank, target[first + i].astype(F32), ids[pl.ds(peer, 1), :]
            )

    pending = []
    for step in range(len(BOUNDS) - 1):
        weight_copy(step).wait()
        products = []
        for group in range(BOUNDS[step], BOUNDS[step + 1]):
            first = group * GROUP
            rhs = jnp.concatenate([jnp.where(column == i, turned[group], 0.0).astype(BF16) for i in range(GROUP)], axis=0)
            parts = [two_parts(weight[first + i]) for i in range(GROUP)]
            product = sum(
                jnp.dot(jnp.concatenate([part[which] for part in parts], axis=1), rhs, preferred_element_type=F32)
                for which in range(2)
            )
            products.append((first, product))
            if pending:
                place(*pending.pop(0))
        if step == 0:
            for index in range(1, layers):
                layer_copy(index).wait()
            tail = jnp.zeros((rows, faces), F32)
            wide = lax.broadcasted_iota(jnp.int32, (rows, faces), 1)
            for degree in range(ORDERS):
                for which in range(layers):
                    spot = degree * layers + which
                    tail = jnp.where(wide == spot, pltpu.roll(moments[degree, which], spot + 1, 1), tail)
            rim[...] = tail.T[: ORDERS * layers]
        for item in pending:
            place(*item)
        pending = products
    for item in pending:
        place(*item)

    for peer in range(peers):
        out[pl.ds(peer * block + ORDERS * cap, 1), :] = ids[pl.ds(peer, 1), :]


def dispatch(owner, target, moments, weight, peers, cap):
    layers, rows, faces = moments.shape[1:]
    return pl.pallas_call(
        functools.partial(dispatch_body, cap),
        out_shape=(
            jax.ShapeDtypeStruct((peers * (ORDERS * cap + 1), faces), F32),
            jax.ShapeDtypeStruct((ORDERS * layers, rows), F32),
        ),
        in_specs=[IN_HBM] * 4,
        out_specs=(IN_VMEM, IN_VMEM),
        scratch_shapes=[
            pltpu.VMEM(moments.shape, F32),
            pltpu.VMEM((rows, faces, faces), F32),
            pltpu.VMEM((PAD * rows, faces), F32),
            pltpu.VMEM((peers, faces), F32),
            pltpu.SMEM((rows,), jnp.int32),
            pltpu.SMEM((rows,), jnp.int32),
            pltpu.SMEM((peers,), jnp.int32),
            pltpu.SemaphoreType.DMA((2,)),
            pltpu.SemaphoreType.DMA((layers,)),
            pltpu.SemaphoreType.DMA((len(BOUNDS) - 1,)),
        ],
        compiler_params=pltpu.CompilerParams(vmem_limit_bytes=FULL_VMEM),
        name="dispatch",
    )(owner, target, moments, weight)


def local_body(
    moments_hbm, rim, azim_hbm, radial_hbm, axial_hbm, shear_hbm, out, edge,
    moments, azim, radial, axial, shear, adv, result, sems, load_sems,
):
    layers, rows, faces = moments.shape[1:]
    loads = [
        pltpu.make_async_copy(source, target, load_sems.at[index])
        for index, (source, target) in enumerate(
            ((moments_hbm, moments), (azim_hbm, azim), (radial_hbm, radial), (axial_hbm, axial), (shear_hbm, shear))
        )
    ]
    for load in loads:
        load.start()
    for load in loads:
        load.wait()
    rotor = lax.axis_index("region") == 0
    interface = jnp.where(rotor, layers - 1, 0)
    row = lax.broadcasted_iota(jnp.int32, (rows, faces), 0)
    lane = lax.broadcasted_iota(jnp.int32, (rows, faces), 1)

    def advect(layer, target):
        ca = azim[layer]
        cr = radial[layer]
        cz = axial[layer]
        outward = jnp.maximum(cr, 0.0)
        inward = outward - cr
        upward = jnp.maximum(cz, 0.0)
        downward = upward - cz
        keep = 1.0 - ca - (outward + inward) - (upward + downward)
        outward = jnp.where(layer > 0, outward, 0.0)
        inward = jnp.where(layer < layers - 1, inward, 0.0)
        upward = jnp.where(row > 0, upward, 0.0)
        downward = jnp.where(row < rows - 1, downward, 0.0)
        below = jnp.maximum(layer - 1, 0)
        beyond = jnp.minimum(layer + 1, layers - 1)
        for degree in range(ORDERS):
            m = moments[degree, layer]
            prev = jnp.where(lane == 0, rim[degree, layer], pltpu.roll(m, 1, 1))
            target[degree] = (
                keep * m
                + ca * prev
                + outward * moments[degree, below]
                + inward * moments[degree, beyond]
                + upward * pltpu.roll(m, 1, 0)
                + downward * pltpu.roll(m, rows - 1, 0)
            )

    def store(index, layer):
        return pltpu.make_async_copy(result.at[index], out.at[:, layer], sems.at[index])

    @pl.loop(0, layers - 1)
    def _(index):
        layer = jnp.where(rotor, index, index + 1)
        advect(layer, adv)

        @pl.loop(0, rows // TILE)
        def _(step):
            part = pl.ds(pl.multiple_of(step * TILE, TILE), TILE)
            updated = sources([adv[degree, part] for degree in range(ORDERS)], shear[layer, part])
            for degree in range(ORDERS):
                result[index, degree, part] = updated[degree]

        store(index, layer).start()

    advect(interface, edge)
    outward = jnp.maximum(radial[interface], 0.0)
    edge[ORDERS] = jnp.where(rotor, outward - radial[interface], outward)
    edge[ORDERS + 1] = shear[interface]

    @pl.loop(0, layers - 1)
    def _(index):
        store(index, jnp.where(rotor, index, index + 1)).wait()


def local_update(moments, rim, azim, radial, axial, shear):
    layers, rows, faces = moments.shape[1:]
    return pl.pallas_call(
        local_body,
        out_shape=(
            jax.ShapeDtypeStruct(moments.shape, F32),
            jax.ShapeDtypeStruct((ORDERS + 2, rows, faces), F32),
        ),
        in_specs=[IN_HBM, IN_VMEM] + [IN_HBM] * 4,
        out_specs=(IN_HBM, IN_VMEM),
        scratch_shapes=[pltpu.VMEM(moments.shape, F32)]
        + [pltpu.VMEM(azim.shape, F32)] * 4
        + [
            pltpu.VMEM((ORDERS, rows, faces), F32),
            pltpu.VMEM((layers - 1, ORDERS, rows, faces), F32),
            pltpu.SemaphoreType.DMA((layers - 1,)),
            pltpu.SemaphoreType.DMA((5,)),
        ],
        compiler_params=pltpu.CompilerParams(vmem_limit_bytes=FULL_VMEM),
        name="local_update",
    )(moments, rim, azim, radial, axial, shear)


def collect_body(peers, cap, received, out, gathered):
    rows, faces = out.shape[1], out.shape[2]
    block = ORDERS * cap + 1
    per_row = faces // cap
    row_id = lax.broadcasted_iota(jnp.int32, (rows, faces), 0).astype(F32)
    hits = []
    for first in range(0, peers, per_row):
        ids = jnp.zeros((1, faces), F32)
        for peer in range(first, min(peers, first + per_row)):
            ids = ids + received[pl.ds(peer * block + ORDERS * cap, 1), :]
        hits.append((row_id == ids).astype(BF16))
    hits = jnp.concatenate(hits, axis=1)
    for degree in range(ORDERS):
        for peer in range(peers):
            gathered[pl.ds(peer * cap, cap), :] = received[pl.ds(peer * block + degree, cap, stride=ORDERS), :]
        high, low = two_parts(gathered[...])
        out[degree] = jnp.dot(hits, high, preferred_element_type=F32) + jnp.dot(
            hits, low, preferred_element_type=F32
        )


def collect(received, rows, peers, cap):
    faces = received.shape[1]
    return pl.pallas_call(
        functools.partial(collect_body, peers, cap),
        out_shape=jax.ShapeDtypeStruct((ORDERS, rows, faces), F32),
        in_specs=[IN_VMEM],
        out_specs=IN_VMEM,
        scratch_shapes=[pltpu.VMEM((peers * cap, faces), F32)],
        compiler_params=pltpu.CompilerParams(vmem_limit_bytes=KERNEL_VMEM),
        name="collect",
    )(received)


def interface_body(before, edge, ghost, out, result, sems):
    rows = ghost.shape[1]
    tiles = sems.shape[0]
    tile = rows // tiles
    layer = jnp.where(lax.axis_index("region") == 0, out.shape[1] - 1, 0)

    def store(step):
        part = pl.ds(step * tile, tile)
        return pltpu.make_async_copy(result.at[:, part], out.at[:, layer, part], sems.at[step])

    for step in range(tiles):
        part = pl.ds(step * tile, tile)
        share = edge[ORDERS, part]
        moment = [edge[degree, part] + share * ghost[degree, part] for degree in range(ORDERS)]
        updated = sources(moment, edge[ORDERS + 1, part])
        for degree in range(ORDERS):
            result[degree, part] = updated[degree]
        store(step).start()
    for step in range(tiles):
        store(step).wait()


def interface_update(before, edge, ghost):
    rows, faces = ghost.shape[1:]
    tiles = rows // TILE
    return pl.pallas_call(
        interface_body,
        out_shape=jax.ShapeDtypeStruct(before.shape, F32),
        in_specs=[IN_HBM, IN_VMEM, IN_VMEM],
        out_specs=IN_HBM,
        scratch_shapes=[pltpu.VMEM((ORDERS, rows, faces), F32), pltpu.SemaphoreType.DMA((tiles,))],
        input_output_aliases={0: 0},
        compiler_params=pltpu.CompilerParams(vmem_limit_bytes=KERNEL_VMEM),
        name="interface_update",
    )(before, edge, ghost)


def on_device(
    moments, courant_azimuth, courant_radial, courant_axial, shear, owner, target, ami_weight
):
    moment = moments[0]
    rows, faces = moment.shape[2], moment.shape[3]
    peers = lax.axis_size("cells")
    regions = lax.axis_size("region")
    cap = max(2, 2 * rows // peers)
    payload, tail = dispatch(owner[0, :, 0], target[0], moment, ami_weight[0], peers, cap)
    received = lax.all_to_all(
        payload.reshape(peers, 1, -1), "cells", split_axis=0, concat_axis=0, tiled=True
    )
    rim = lax.ppermute(tail, "cells", [(i, (i + 1) % peers) for i in range(peers)])
    rim = rim.reshape(ORDERS, -1, rows)
    before, edge = local_update(
        moment, rim[..., None], courant_azimuth[0], courant_radial[0], courant_axial[0], shear[0]
    )
    other = collect(received.reshape(-1, faces), rows, peers, cap)
    ghost = lax.ppermute(other, "region", [(i, regions - 1 - i) for i in range(regions)])
    updated = interface_update(before, edge, ghost)
    return updated[None]


def solution(mesh):
    field = P("region", None, None, "cells")
    cells = P("region", None, None, None, "cells")
    return jax.shard_map(
        on_device,
        mesh=mesh,
        in_specs=(
            cells,
            field,
            field,
            field,
            field,
            P("region", "cells", None),
            P("region", "cells"),
            P("region", "cells", None, None),
        ),
        out_specs=cells,
        check_vma=False,
    )
```

```python
import functools
import math

import jax
import jax.numpy as jnp
from jax import lax
from jax.experimental import pallas as pl
from jax.experimental.pallas import tpu as pltpu
from jax.sharding import PartitionSpec as P


KAGG = 0.005
KBRK = 0.02
ORDERS = 6
F32 = jnp.float32
BF16 = jnp.bfloat16
KERNEL_VMEM = 8 * 1024 * 1024
PAD = 8
GROUP = 8
TILE = 32
FULL_VMEM = 58 * 1024 * 1024
BOUNDS = (0, 2, 5, 8, 11, 14, 16)
AHEAD = 3
RIM_STEP = 3
IN_VMEM = pl.BlockSpec(memory_space=pltpu.VMEM)
IN_HBM = pl.BlockSpec(memory_space=pltpu.HBM)

COS_THIRD = (
    0.44444444535893496,
    0.04115211563399856,
    0.009758495429256357,
    0.0029417445898478234,
    0.0012216398155368902,
    -0.00013418618671007774,
    0.0009423656998505278,
    -0.000598812660480466,
    0.00027219066323123,
)


def two_parts(value):
    high = value.astype(BF16)
    return high, (value - high.astype(F32)).astype(BF16)


def quadrature(moment):
    inv_mass = 1.0 / moment[0]
    n1, n2, n3, n4, n5 = [moment[degree] * inv_mass for degree in range(1, 6)]
    p1 = n2 - n1 * n1
    p2 = n3 - n1 * n2
    p3 = n4 - n1 * n3
    p4 = n5 - n1 * n4
    inv_p1 = 1.0 / p1
    slope = p2 * inv_p1
    a1 = slope - n1
    q2 = p3 - a1 * p2 - p1 * n2
    q3 = p4 - a1 * p3 - p1 * n3
    inv_q2 = 1.0 / q2
    a2 = q3 * inv_q2 - slope
    b2 = q2 * inv_p1
    centre = (n1 + a1 + a2) * (1.0 / 3.0)
    d0 = n1 - centre
    d1 = a1 - centre
    d2 = a2 - centre
    square = (d0 * d0 + d1 * d1 + d2 * d2 + 2.0 * (p1 + b2)) * (1.0 / 6.0)
    inv_h = lax.rsqrt(square)
    h = square * inv_h
    determ = d0 * (d1 * d2 - b2) - p1 * d2
    cosine = jnp.clip(determ * 0.5 * (inv_h * inv_h * inv_h), -1.0, 1.0)
    half = jnp.sqrt(0.5 + 0.5 * cosine)
    w = (0.5 - 0.5 * cosine) / (1.0 + half)
    q = jnp.full_like(w, COS_THIRD[-1])
    for term in COS_THIRD[-2::-1]:
        q = q * w + term
    drop = w * q
    h_cos = h * (1.0 - drop)
    h_sin = h * jnp.sqrt(drop * (2.0 - drop)) * math.sqrt(3.0)
    high = centre + 2.0 * h_cos
    low = centre - h_cos - h_sin
    mid = 3.0 * centre - high - low
    nodes = (low, mid, high)
    weights = []
    for node in nodes:
        u = node - n1
        v = (node - a1) * u - p1
        weights.append(moment[0] / (1.0 + u * u * inv_p1 + v * v * inv_q2))
    return nodes, weights


def sources(moment, shear):
    nodes, weights = quadrature(moment)
    cubes = [node * node * node for node in nodes]
    rate = KBRK * shear
    agg = KAGG * shear
    breaks = [weights[i] * rate * cubes[i] for i in range(3)]
    equal = [weights[i] * agg * (4.0 * cubes[i]) * weights[i] for i in range(3)]
    lost = [2.0 * equal[i] for i in range(3)]
    pairs = []
    for i, j in ((0, 1), (0, 2), (1, 2)):
        summed = nodes[i] + nodes[j]
        pair = weights[i] * weights[j] * (agg * summed * summed * summed)
        lost[i] = lost[i] + pair
        lost[j] = lost[j] + pair
        volume = cubes[i] + cubes[j]
        root = jnp.exp(jnp.log(volume) * (1.0 / 3.0))
        pairs.append((pair, root, volume))
    updated = []
    node_powers = [jnp.ones_like(shear)] * 3
    for degree in range(ORDERS):
        grow = 2.0 ** (degree / 3.0)
        split = 2.0 ** (1.0 - degree / 3.0) - 1.0
        total = moment[degree]
        for i in range(3):
            net = grow * equal[i] - lost[i]
            if degree != 3:
                net = net + split * breaks[i]
            if degree > 0:
                net = net * node_powers[i]
            total = total + net
        for pair, root, volume in pairs:
            factor = (None, root, root * root, volume, volume * root, volume * root * root)[degree]
            total = total + (pair if factor is None else pair * factor)
        updated.append(total)
        node_powers = [power * node for power, node in zip(node_powers, nodes)] if degree else list(nodes)
    return updated


def dispatch_body(
    cap, owner_hbm, target_hbm, moments_hbm, weight_hbm, out, rim,
    moments, weight, source, ids, owner, target, count, index_sem, moment_sem, weight_sem,
):
    layers, rows, faces = moments.shape[1:]
    peers = count.shape[0]
    block = ORDERS * cap + 1
    rotor = lax.axis_index("region") == 0
    layer = jnp.where(rotor, layers - 1, 0)

    def layer_copy(index):
        which = jnp.where(rotor, layers - 1 - index, index)
        return pltpu.make_async_copy(moments_hbm.at[:, which], moments.at[:, which], moment_sem.at[index])

    def weight_copy(step):
        part = pl.ds(BOUNDS[step] * rows // BOUNDS[-1], (BOUNDS[step + 1] - BOUNDS[step]) * rows // BOUNDS[-1])
        return pltpu.make_async_copy(weight_hbm.at[part], weight.at[part], weight_sem.at[step])

    index_copies = (
        pltpu.make_async_copy(owner_hbm, owner, index_sem.at[0]),
        pltpu.make_async_copy(target_hbm, target, index_sem.at[1]),
    )
    layer_copy(0).start()
    for copy in index_copies:
        copy.start()

    out[...] = jnp.zeros_like(out)
    lane = lax.broadcasted_iota(jnp.int32, (1, faces), 1)
    offset = (lax.axis_index("cells") * cap) % faces
    mine = jnp.logical_and(lane >= offset, lane < offset + cap)
    ids[...] = jnp.broadcast_to(jnp.where(mine, -1.0, 0.0), ids.shape)

    @pl.loop(0, peers)
    def _(peer):
        count[peer] = 0

    source[pl.ds(ORDERS * rows, (PAD - ORDERS) * rows)] = jnp.zeros(((PAD - ORDERS) * rows, faces), F32)
    layer_copy(0).wait()
    for step in range(AHEAD):
        weight_copy(step).start()
    for degree in range(ORDERS):
        source[pl.ds(degree * rows, rows)] = moments[degree, layer]
    for copy in index_copies:
        copy.wait()
    width = PAD * GROUP
    column = (lax.broadcasted_iota(jnp.int32, (faces, 2 * width), 1) % width) // PAD
    turned = []
    for first in range(0, rows, GROUP):
        value = jnp.concatenate([source[pl.ds(first + i, PAD, stride=rows)] for i in range(GROUP)], axis=0)
        high = value.astype(BF16).astype(F32)
        turned.append(jnp.concatenate([high, value - high], axis=0).T)

    def place(first, product):
        product = product.T
        product = product[:width] + product[width:]
        for i in range(GROUP):
            peer = owner[first + i]
            rank = count[peer]
            count[peer] = rank + 1
            out[pl.ds(peer * block + rank * ORDERS, ORDERS), :] = product[PAD * i : PAD * i + ORDERS]
            ids[pl.ds(peer, 1), :] = jnp.where(
                lane == offset + rank, target[first + i].astype(F32), ids[pl.ds(peer, 1), :]
            )

    pending = []
    for step in range(len(BOUNDS) - 1):
        weight_copy(step).wait()
        if step + AHEAD < len(BOUNDS) - 1:
            weight_copy(step + AHEAD).start()
        if step == 0:
            for index in range(1, layers):
                layer_copy(index).start()
        products = []
        for group in range(BOUNDS[step], BOUNDS[step + 1]):
            first = group * GROUP
            rhs = jnp.concatenate([jnp.where(column == i, turned[group], 0.0).astype(BF16) for i in range(GROUP)], axis=0)
            parts = [two_parts(weight[first + i]) for i in range(GROUP)]
            product = sum(
                jnp.dot(jnp.concatenate([part[which] for part in parts], axis=1), rhs, preferred_element_type=F32)
                for which in range(2)
            )
            products.append((first, product))
            if pending:
                place(*pending.pop(0))
        if step == RIM_STEP:
            for index in range(1, layers):
                layer_copy(index).wait()
            tail = jnp.zeros((rows, faces), F32)
            wide = lax.broadcasted_iota(jnp.int32, (rows, faces), 1)
            for degree in range(ORDERS):
                for which in range(layers):
                    spot = degree * layers + which
                    tail = jnp.where(wide == spot, pltpu.roll(moments[degree, which], spot + 1, 1), tail)
            rim[...] = tail.T[: ORDERS * layers]
        for item in pending:
            place(*item)
        pending = products
    for item in pending:
        place(*item)

    for peer in range(peers):
        out[pl.ds(peer * block + ORDERS * cap, 1), :] = ids[pl.ds(peer, 1), :]


def dispatch(owner, target, moments, weight, peers, cap):
    layers, rows, faces = moments.shape[1:]
    return pl.pallas_call(
        functools.partial(dispatch_body, cap),
        out_shape=(
            jax.ShapeDtypeStruct((peers * (ORDERS * cap + 1), faces), F32),
            jax.ShapeDtypeStruct((ORDERS * layers, rows), F32),
        ),
        in_specs=[IN_HBM] * 4,
        out_specs=(IN_VMEM, IN_VMEM),
        scratch_shapes=[
            pltpu.VMEM(moments.shape, F32),
            pltpu.VMEM((rows, faces, faces), F32),
            pltpu.VMEM((PAD * rows, faces), F32),
            pltpu.VMEM((peers, faces), F32),
            pltpu.SMEM((rows,), jnp.int32),
            pltpu.SMEM((rows,), jnp.int32),
            pltpu.SMEM((peers,), jnp.int32),
            pltpu.SemaphoreType.DMA((2,)),
            pltpu.SemaphoreType.DMA((layers,)),
            pltpu.SemaphoreType.DMA((len(BOUNDS) - 1,)),
        ],
        compiler_params=pltpu.CompilerParams(vmem_limit_bytes=FULL_VMEM),
        name="dispatch",
    )(owner, target, moments, weight)


def local_body(
    moments_hbm, rim, azim_hbm, radial_hbm, axial_hbm, shear_hbm, out, edge,
    moments, azim, radial, axial, shear, adv, result, sems, load_sems,
):
    layers, rows, faces = moments.shape[1:]
    loads = [
        pltpu.make_async_copy(source, target, load_sems.at[index])
        for index, (source, target) in enumerate(
            ((moments_hbm, moments), (azim_hbm, azim), (radial_hbm, radial), (axial_hbm, axial), (shear_hbm, shear))
        )
    ]
    for load in loads:
        load.start()
    for load in loads:
        load.wait()
    rotor = lax.axis_index("region") == 0
    interface = jnp.where(rotor, layers - 1, 0)
    row = lax.broadcasted_iota(jnp.int32, (rows, faces), 0)
    lane = lax.broadcasted_iota(jnp.int32, (rows, faces), 1)

    def advect(layer, target):
        ca = azim[layer]
        cr = radial[layer]
        cz = axial[layer]
        outward = jnp.maximum(cr, 0.0)
        inward = outward - cr
        upward = jnp.maximum(cz, 0.0)
        downward = upward - cz
        keep = 1.0 - ca - (outward + inward) - (upward + downward)
        outward = jnp.where(layer > 0, outward, 0.0)
        inward = jnp.where(layer < layers - 1, inward, 0.0)
        upward = jnp.where(row > 0, upward, 0.0)
        downward = jnp.where(row < rows - 1, downward, 0.0)
        below = jnp.maximum(layer - 1, 0)
        beyond = jnp.minimum(layer + 1, layers - 1)
        for degree in range(ORDERS):
            m = moments[degree, layer]
            prev = jnp.where(lane == 0, rim[degree, layer], pltpu.roll(m, 1, 1))
            target[degree] = (
                keep * m
                + ca * prev
                + outward * moments[degree, below]
                + inward * moments[degree, beyond]
                + upward * pltpu.roll(m, 1, 0)
                + downward * pltpu.roll(m, rows - 1, 0)
            )

    def store(index, layer):
        return pltpu.make_async_copy(result.at[index], out.at[:, layer], sems.at[index])

    @pl.loop(0, layers - 1)
    def _(index):
        layer = jnp.where(rotor, index, index + 1)
        advect(layer, adv)

        @pl.loop(0, rows // TILE)
        def _(step):
            part = pl.ds(pl.multiple_of(step * TILE, TILE), TILE)
            updated = sources([adv[degree, part] for degree in range(ORDERS)], shear[layer, part])
            for degree in range(ORDERS):
                result[index, degree, part] = updated[degree]

        store(index, layer).start()

    advect(interface, edge)
    outward = jnp.maximum(radial[interface], 0.0)
    edge[ORDERS] = jnp.where(rotor, outward - radial[interface], outward)
    edge[ORDERS + 1] = shear[interface]

    @pl.loop(0, layers - 1)
    def _(index):
        store(index, jnp.where(rotor, index, index + 1)).wait()


def local_update(moments, rim, azim, radial, axial, shear):
    layers, rows, faces = moments.shape[1:]
    return pl.pallas_call(
        local_body,
        out_shape=(
            jax.ShapeDtypeStruct(moments.shape, F32),
            jax.ShapeDtypeStruct((ORDERS + 2, rows, faces), F32),
        ),
        in_specs=[IN_HBM, IN_VMEM] + [IN_HBM] * 4,
        out_specs=(IN_HBM, IN_VMEM),
        scratch_shapes=[pltpu.VMEM(moments.shape, F32)]
        + [pltpu.VMEM(azim.shape, F32)] * 4
        + [
            pltpu.VMEM((ORDERS, rows, faces), F32),
            pltpu.VMEM((layers - 1, ORDERS, rows, faces), F32),
            pltpu.SemaphoreType.DMA((layers - 1,)),
            pltpu.SemaphoreType.DMA((5,)),
        ],
        compiler_params=pltpu.CompilerParams(vmem_limit_bytes=FULL_VMEM),
        name="local_update",
    )(moments, rim, azim, radial, axial, shear)


def collect_body(peers, cap, received, out, gathered):
    rows, faces = out.shape[1], out.shape[2]
    block = ORDERS * cap + 1
    per_row = faces // cap
    row_id = lax.broadcasted_iota(jnp.int32, (rows, faces), 0).astype(F32)
    hits = []
    for first in range(0, peers, per_row):
        ids = jnp.zeros((1, faces), F32)
        for peer in range(first, min(peers, first + per_row)):
            ids = ids + received[pl.ds(peer * block + ORDERS * cap, 1), :]
        hits.append((row_id == ids).astype(BF16))
    hits = jnp.concatenate(hits, axis=1)
    for degree in range(ORDERS):
        for peer in range(peers):
            gathered[pl.ds(peer * cap, cap), :] = received[pl.ds(peer * block + degree, cap, stride=ORDERS), :]
        high, low = two_parts(gathered[...])
        out[degree] = jnp.dot(hits, high, preferred_element_type=F32) + jnp.dot(
            hits, low, preferred_element_type=F32
        )


def collect(received, rows, peers, cap):
    faces = received.shape[1]
    return pl.pallas_call(
        functools.partial(collect_body, peers, cap),
        out_shape=jax.ShapeDtypeStruct((ORDERS, rows, faces), F32),
        in_specs=[IN_VMEM],
        out_specs=IN_VMEM,
        scratch_shapes=[pltpu.VMEM((peers * cap, faces), F32)],
        compiler_params=pltpu.CompilerParams(vmem_limit_bytes=KERNEL_VMEM),
        name="collect",
    )(received)


def fetch_body(source, out, sem):
    copy = pltpu.make_async_copy(source, out, sem)
    copy.start()
    copy.wait()


def fetch(edge):
    return pl.pallas_call(
        fetch_body,
        out_shape=jax.ShapeDtypeStruct(edge.shape, F32),
        in_specs=[IN_HBM],
        out_specs=IN_VMEM,
        scratch_shapes=[pltpu.SemaphoreType.DMA],
        compiler_params=pltpu.CompilerParams(vmem_limit_bytes=KERNEL_VMEM),
        name="fetch",
    )(edge)


def interface_body(before, edge, ghost, out, result, sems):
    rows = ghost.shape[1]
    tiles = sems.shape[0]
    tile = rows // tiles
    layer = jnp.where(lax.axis_index("region") == 0, out.shape[1] - 1, 0)

    def store(step):
        part = pl.ds(step * tile, tile)
        return pltpu.make_async_copy(result.at[:, part], out.at[:, layer, part], sems.at[step])

    for step in range(tiles):
        part = pl.ds(step * tile, tile)
        share = edge[ORDERS, part]
        moment = [edge[degree, part] + share * ghost[degree, part] for degree in range(ORDERS)]
        updated = sources(moment, edge[ORDERS + 1, part])
        for degree in range(ORDERS):
            result[degree, part] = updated[degree]
        store(step).start()
    for step in range(tiles):
        store(step).wait()


def interface_update(before, edge, ghost):
    rows, faces = ghost.shape[1:]
    tiles = rows // TILE
    return pl.pallas_call(
        interface_body,
        out_shape=jax.ShapeDtypeStruct(before.shape, F32),
        in_specs=[IN_HBM, IN_VMEM, IN_VMEM],
        out_specs=IN_HBM,
        scratch_shapes=[pltpu.VMEM((ORDERS, rows, faces), F32), pltpu.SemaphoreType.DMA((tiles,))],
        input_output_aliases={0: 0},
        compiler_params=pltpu.CompilerParams(vmem_limit_bytes=KERNEL_VMEM),
        name="interface_update",
    )(before, edge, ghost)


def on_device(
    moments, courant_azimuth, courant_radial, courant_axial, shear, owner, target, ami_weight
):
    moment = moments[0]
    rows, faces = moment.shape[2], moment.shape[3]
    peers = lax.axis_size("cells")
    regions = lax.axis_size("region")
    cap = max(2, 2 * rows // peers)
    payload, tail = dispatch(owner[0, :, 0], target[0], moment, ami_weight[0], peers, cap)
    received = lax.all_to_all(
        payload.reshape(peers, 1, -1), "cells", split_axis=0, concat_axis=0, tiled=True
    )
    rim = lax.ppermute(tail, "cells", [(i, (i + 1) % peers) for i in range(peers)])
    rim = rim.reshape(ORDERS, -1, rows)
    before, edge = local_update(
        moment, rim[..., None], courant_azimuth[0], courant_radial[0], courant_axial[0], shear[0]
    )
    other = collect(received.reshape(-1, faces), rows, peers, cap)
    ghost = lax.ppermute(other, "region", [(i, regions - 1 - i) for i in range(regions)])
    edge = fetch(edge)
    updated = interface_update(before, edge, ghost)
    return updated[None]


def solution(mesh):
    field = P("region", None, None, "cells")
    cells = P("region", None, None, None, "cells")
    return jax.shard_map(
        on_device,
        mesh=mesh,
        in_specs=(
            cells,
            field,
            field,
            field,
            field,
            P("region", "cells", None),
            P("region", "cells"),
            P("region", "cells", None, None),
        ),
        out_specs=cells,
        check_vma=False,
    )
```

```python
import functools
import math

import jax
import jax.numpy as jnp
from jax import lax
from jax.experimental import pallas as pl
from jax.experimental.pallas import tpu as pltpu
from jax.sharding import PartitionSpec as P


KAGG = 0.005
KBRK = 0.02
ORDERS = 6
F32 = jnp.float32
BF16 = jnp.bfloat16
KERNEL_VMEM = 8 * 1024 * 1024
PAD = 8
GROUP = 8
TILE = 32
EDGE_TILE = 32
FULL_VMEM = 58 * 1024 * 1024
BOUNDS = (0, 2, 5, 8, 11, 14, 16)
AHEAD = 3
RIM_STEP = 3
IN_VMEM = pl.BlockSpec(memory_space=pltpu.VMEM)
IN_HBM = pl.BlockSpec(memory_space=pltpu.HBM)

COS_THIRD = (
    0.44444444535893496,
    0.04115211563399856,
    0.009758495429256357,
    0.0029417445898478234,
    0.0012216398155368902,
    -0.00013418618671007774,
    0.0009423656998505278,
    -0.000598812660480466,
    0.00027219066323123,
)


def two_parts(value):
    high = value.astype(BF16)
    return high, (value - high.astype(F32)).astype(BF16)


def quadrature(moment):
    inv_mass = 1.0 / moment[0]
    n1, n2, n3, n4, n5 = [moment[degree] * inv_mass for degree in range(1, 6)]
    p1 = n2 - n1 * n1
    p2 = n3 - n1 * n2
    p3 = n4 - n1 * n3
    p4 = n5 - n1 * n4
    inv_p1 = 1.0 / p1
    slope = p2 * inv_p1
    a1 = slope - n1
    q2 = p3 - a1 * p2 - p1 * n2
    q3 = p4 - a1 * p3 - p1 * n3
    inv_q2 = 1.0 / q2
    a2 = q3 * inv_q2 - slope
    b2 = q2 * inv_p1
    centre = (n1 + a1 + a2) * (1.0 / 3.0)
    d0 = n1 - centre
    d1 = a1 - centre
    d2 = a2 - centre
    square = (d0 * d0 + d1 * d1 + d2 * d2 + 2.0 * (p1 + b2)) * (1.0 / 6.0)
    inv_h = lax.rsqrt(square)
    h = square * inv_h
    determ = d0 * (d1 * d2 - b2) - p1 * d2
    cosine = jnp.clip(determ * 0.5 * (inv_h * inv_h * inv_h), -1.0, 1.0)
    half = jnp.sqrt(0.5 + 0.5 * cosine)
    w = (0.5 - 0.5 * cosine) / (1.0 + half)
    q = jnp.full_like(w, COS_THIRD[-1])
    for term in COS_THIRD[-2::-1]:
        q = q * w + term
    drop = w * q
    h_cos = h * (1.0 - drop)
    h_sin = h * jnp.sqrt(drop * (2.0 - drop)) * math.sqrt(3.0)
    high = centre + 2.0 * h_cos
    low = centre - h_cos - h_sin
    mid = 3.0 * centre - high - low
    nodes = (low, mid, high)
    weights = []
    for node in nodes:
        u = node - n1
        v = (node - a1) * u - p1
        weights.append(moment[0] / (1.0 + u * u * inv_p1 + v * v * inv_q2))
    return nodes, weights


def sources(moment, shear):
    nodes, weights = quadrature(moment)
    cubes = [node * node * node for node in nodes]
    rate = KBRK * shear
    agg = KAGG * shear
    breaks = [weights[i] * rate * cubes[i] for i in range(3)]
    equal = [weights[i] * agg * (4.0 * cubes[i]) * weights[i] for i in range(3)]
    lost = [2.0 * equal[i] for i in range(3)]
    pairs = []
    for i, j in ((0, 1), (0, 2), (1, 2)):
        summed = nodes[i] + nodes[j]
        pair = weights[i] * weights[j] * (agg * summed * summed * summed)
        lost[i] = lost[i] + pair
        lost[j] = lost[j] + pair
        volume = cubes[i] + cubes[j]
        root = jnp.exp(jnp.log(volume) * (1.0 / 3.0))
        pairs.append((pair, root, volume))
    updated = []
    node_powers = [jnp.ones_like(shear)] * 3
    for degree in range(ORDERS):
        grow = 2.0 ** (degree / 3.0)
        split = 2.0 ** (1.0 - degree / 3.0) - 1.0
        total = moment[degree]
        for i in range(3):
            net = grow * equal[i] - lost[i]
            if degree != 3:
                net = net + split * breaks[i]
            if degree > 0:
                net = net * node_powers[i]
            total = total + net
        for pair, root, volume in pairs:
            factor = (None, root, root * root, volume, volume * root, volume * root * root)[degree]
            total = total + (pair if factor is None else pair * factor)
        updated.append(total)
        node_powers = [power * node for power, node in zip(node_powers, nodes)] if degree else list(nodes)
    return updated


def dispatch_body(
    cap, owner_hbm, target_hbm, moments_hbm, weight_hbm, out, rim,
    moments, weight, source, ids, owner, target, count, index_sem, moment_sem, weight_sem,
):
    layers, rows, faces = moments.shape[1:]
    peers = count.shape[0]
    block = ORDERS * cap + 1
    rotor = lax.axis_index("region") == 0
    layer = jnp.where(rotor, layers - 1, 0)

    def layer_copy(index):
        which = jnp.where(rotor, layers - 1 - index, index)
        return pltpu.make_async_copy(moments_hbm.at[:, which], moments.at[:, which], moment_sem.at[index])

    def weight_copy(step):
        part = pl.ds(BOUNDS[step] * rows // BOUNDS[-1], (BOUNDS[step + 1] - BOUNDS[step]) * rows // BOUNDS[-1])
        return pltpu.make_async_copy(weight_hbm.at[part], weight.at[part], weight_sem.at[step])

    index_copies = (
        pltpu.make_async_copy(owner_hbm, owner, index_sem.at[0]),
        pltpu.make_async_copy(target_hbm, target, index_sem.at[1]),
    )
    layer_copy(0).start()
    for step in range(AHEAD):
        weight_copy(step).start(priority=1)
    for copy in index_copies:
        copy.start()

    out[...] = jnp.zeros_like(out)
    lane = lax.broadcasted_iota(jnp.int32, (1, faces), 1)
    offset = (lax.axis_index("cells") * cap) % faces
    mine = jnp.logical_and(lane >= offset, lane < offset + cap)
    ids[...] = jnp.broadcast_to(jnp.where(mine, -1.0, 0.0), ids.shape)

    @pl.loop(0, peers)
    def _(peer):
        count[peer] = 0

    source[pl.ds(ORDERS * rows, (PAD - ORDERS) * rows)] = jnp.zeros(((PAD - ORDERS) * rows, faces), F32)
    layer_copy(0).wait()
    for degree in range(ORDERS):
        source[pl.ds(degree * rows, rows)] = moments[degree, layer]
    for copy in index_copies:
        copy.wait()
    width = PAD * GROUP
    column = (lax.broadcasted_iota(jnp.int32, (faces, 2 * width), 1) % width) // PAD
    turned = []
    for first in range(0, rows, GROUP):
        value = jnp.concatenate([source[pl.ds(first + i, PAD, stride=rows)] for i in range(GROUP)], axis=0)
        high = value.astype(BF16).astype(F32)
        turned.append(jnp.concatenate([high, value - high], axis=0).T)

    def place(first, product):
        product = product.T
        product = product[:width] + product[width:]
        for i in range(GROUP):
            peer = owner[first + i]
            rank = count[peer]
            count[peer] = rank + 1
            out[pl.ds(peer * block + rank * ORDERS, ORDERS), :] = product[PAD * i : PAD * i + ORDERS]
            ids[pl.ds(peer, 1), :] = jnp.where(
                lane == offset + rank, target[first + i].astype(F32), ids[pl.ds(peer, 1), :]
            )

    pending = []
    for step in range(len(BOUNDS) - 1):
        weight_copy(step).wait()
        if step + AHEAD < len(BOUNDS) - 1:
            weight_copy(step + AHEAD).start()
        if step == 0:
            for index in range(1, layers):
                layer_copy(index).start()
        products = []
        for group in range(BOUNDS[step], BOUNDS[step + 1]):
            first = group * GROUP
            rhs = jnp.concatenate([jnp.where(column == i, turned[group], 0.0).astype(BF16) for i in range(GROUP)], axis=0)
            parts = [two_parts(weight[first + i]) for i in range(GROUP)]
            product = sum(
                jnp.dot(jnp.concatenate([part[which] for part in parts], axis=1), rhs, preferred_element_type=F32)
                for which in range(2)
            )
            products.append((first, product))
            if pending:
                place(*pending.pop(0))
        if step == RIM_STEP:
            for index in range(1, layers):
                layer_copy(index).wait()
            tail = jnp.zeros((rows, faces), F32)
            wide = lax.broadcasted_iota(jnp.int32, (rows, faces), 1)
            for degree in range(ORDERS):
                for which in range(layers):
                    spot = degree * layers + which
                    tail = jnp.where(wide == spot, pltpu.roll(moments[degree, which], spot + 1, 1), tail)
            rim[...] = tail.T[: ORDERS * layers]
        for item in pending:
            place(*item)
        pending = products
    for item in pending:
        place(*item)

    for peer in range(peers):
        out[pl.ds(peer * block + ORDERS * cap, 1), :] = ids[pl.ds(peer, 1), :]


def dispatch(owner, target, moments, weight, peers, cap):
    layers, rows, faces = moments.shape[1:]
    return pl.pallas_call(
        functools.partial(dispatch_body, cap),
        out_shape=(
            jax.ShapeDtypeStruct((peers * (ORDERS * cap + 1), faces), F32),
            jax.ShapeDtypeStruct((ORDERS * layers, rows), F32),
        ),
        in_specs=[IN_HBM] * 4,
        out_specs=(IN_VMEM, IN_VMEM),
        scratch_shapes=[
            pltpu.VMEM(moments.shape, F32),
            pltpu.VMEM((rows, faces, faces), F32),
            pltpu.VMEM((PAD * rows, faces), F32),
            pltpu.VMEM((peers, faces), F32),
            pltpu.SMEM((rows,), jnp.int32),
            pltpu.SMEM((rows,), jnp.int32),
            pltpu.SMEM((peers,), jnp.int32),
            pltpu.SemaphoreType.DMA((2,)),
            pltpu.SemaphoreType.DMA((layers,)),
            pltpu.SemaphoreType.DMA((len(BOUNDS) - 1,)),
        ],
        compiler_params=pltpu.CompilerParams(vmem_limit_bytes=FULL_VMEM),
        name="dispatch",
    )(owner, target, moments, weight)


def local_body(
    moments_hbm, rim, azim_hbm, radial_hbm, axial_hbm, shear_hbm, out, edge,
    moments, azim, radial, axial, shear, adv, result, sems, load_sems,
):
    layers, rows, faces = moments.shape[1:]
    loads = [
        pltpu.make_async_copy(source, target, load_sems.at[index])
        for index, (source, target) in enumerate(
            ((moments_hbm, moments), (azim_hbm, azim), (radial_hbm, radial), (axial_hbm, axial), (shear_hbm, shear))
        )
    ]
    for load in loads:
        load.start()
    for load in loads:
        load.wait()
    rotor = lax.axis_index("region") == 0
    interface = jnp.where(rotor, layers - 1, 0)
    row = lax.broadcasted_iota(jnp.int32, (rows, faces), 0)
    lane = lax.broadcasted_iota(jnp.int32, (rows, faces), 1)

    def advect(layer, target):
        ca = azim[layer]
        cr = radial[layer]
        cz = axial[layer]
        outward = jnp.maximum(cr, 0.0)
        inward = outward - cr
        upward = jnp.maximum(cz, 0.0)
        downward = upward - cz
        keep = 1.0 - ca - (outward + inward) - (upward + downward)
        outward = jnp.where(layer > 0, outward, 0.0)
        inward = jnp.where(layer < layers - 1, inward, 0.0)
        upward = jnp.where(row > 0, upward, 0.0)
        downward = jnp.where(row < rows - 1, downward, 0.0)
        below = jnp.maximum(layer - 1, 0)
        beyond = jnp.minimum(layer + 1, layers - 1)
        for degree in range(ORDERS):
            m = moments[degree, layer]
            prev = jnp.where(lane == 0, rim[degree, layer], pltpu.roll(m, 1, 1))
            target[degree] = (
                keep * m
                + ca * prev
                + outward * moments[degree, below]
                + inward * moments[degree, beyond]
                + upward * pltpu.roll(m, 1, 0)
                + downward * pltpu.roll(m, rows - 1, 0)
            )

    def store(index, layer):
        return pltpu.make_async_copy(result.at[index], out.at[:, layer], sems.at[index])

    @pl.loop(0, layers - 1)
    def _(index):
        layer = jnp.where(rotor, index, index + 1)
        advect(layer, adv)

        @pl.loop(0, rows // TILE)
        def _(step):
            part = pl.ds(pl.multiple_of(step * TILE, TILE), TILE)
            updated = sources([adv[degree, part] for degree in range(ORDERS)], shear[layer, part])
            for degree in range(ORDERS):
                result[index, degree, part] = updated[degree]

        store(index, layer).start()

    advect(interface, edge)
    outward = jnp.maximum(radial[interface], 0.0)
    edge[ORDERS] = jnp.where(rotor, outward - radial[interface], outward)
    edge[ORDERS + 1] = shear[interface]

    @pl.loop(0, layers - 1)
    def _(index):
        store(index, jnp.where(rotor, index, index + 1)).wait()


def local_update(moments, rim, azim, radial, axial, shear):
    layers, rows, faces = moments.shape[1:]
    return pl.pallas_call(
        local_body,
        out_shape=(
            jax.ShapeDtypeStruct(moments.shape, F32),
            jax.ShapeDtypeStruct((ORDERS + 2, rows, faces), F32),
        ),
        in_specs=[IN_HBM, IN_VMEM] + [IN_HBM] * 4,
        out_specs=(IN_HBM, IN_VMEM),
        scratch_shapes=[pltpu.VMEM(moments.shape, F32)]
        + [pltpu.VMEM(azim.shape, F32)] * 4
        + [
            pltpu.VMEM((ORDERS, rows, faces), F32),
            pltpu.VMEM((layers - 1, ORDERS, rows, faces), F32),
            pltpu.SemaphoreType.DMA((layers - 1,)),
            pltpu.SemaphoreType.DMA((5,)),
        ],
        compiler_params=pltpu.CompilerParams(vmem_limit_bytes=FULL_VMEM),
        name="local_update",
    )(moments, rim, azim, radial, axial, shear)


def collect_body(peers, cap, received, out, gathered):
    rows, faces = out.shape[1], out.shape[2]
    block = ORDERS * cap + 1
    per_row = faces // cap
    row_id = lax.broadcasted_iota(jnp.int32, (rows, faces), 0).astype(F32)
    hits = []
    for first in range(0, peers, per_row):
        ids = jnp.zeros((1, faces), F32)
        for peer in range(first, min(peers, first + per_row)):
            ids = ids + received[pl.ds(peer * block + ORDERS * cap, 1), :]
        hits.append((row_id == ids).astype(BF16))
    hits = jnp.concatenate(hits, axis=1)
    for degree in range(ORDERS):
        for peer in range(peers):
            gathered[pl.ds(peer * cap, cap), :] = received[pl.ds(peer * block + degree, cap, stride=ORDERS), :]
        high, low = two_parts(gathered[...])
        out[degree] = jnp.dot(hits, high, preferred_element_type=F32) + jnp.dot(
            hits, low, preferred_element_type=F32
        )


def collect(received, rows, peers, cap):
    faces = received.shape[1]
    return pl.pallas_call(
        functools.partial(collect_body, peers, cap),
        out_shape=jax.ShapeDtypeStruct((ORDERS, rows, faces), F32),
        in_specs=[IN_VMEM],
        out_specs=IN_VMEM,
        scratch_shapes=[pltpu.VMEM((peers * cap, faces), F32)],
        compiler_params=pltpu.CompilerParams(vmem_limit_bytes=KERNEL_VMEM),
        name="collect",
    )(received)


def fetch_body(source, out, sem):
    copy = pltpu.make_async_copy(source, out, sem)
    copy.start()
    copy.wait()


def fetch(edge):
    return pl.pallas_call(
        fetch_body,
        out_shape=jax.ShapeDtypeStruct(edge.shape, F32),
        in_specs=[IN_HBM],
        out_specs=IN_VMEM,
        scratch_shapes=[pltpu.SemaphoreType.DMA],
        compiler_params=pltpu.CompilerParams(vmem_limit_bytes=KERNEL_VMEM),
        name="fetch",
    )(edge)


def interface_body(before, edge, ghost, out, result, sems):
    rows = ghost.shape[1]
    tiles = sems.shape[0]
    tile = rows // tiles
    layer = jnp.where(lax.axis_index("region") == 0, out.shape[1] - 1, 0)

    def store(step):
        part = pl.ds(step * tile, tile)
        return pltpu.make_async_copy(result.at[:, part], out.at[:, layer, part], sems.at[step])

    for step in range(tiles):
        part = pl.ds(step * tile, tile)
        share = edge[ORDERS, part]
        moment = [edge[degree, part] + share * ghost[degree, part] for degree in range(ORDERS)]
        updated = sources(moment, edge[ORDERS + 1, part])
        for degree in range(ORDERS):
            result[degree, part] = updated[degree]
        store(step).start()
    for step in range(tiles):
        store(step).wait()


def interface_update(before, edge, ghost):
    rows, faces = ghost.shape[1:]
    tiles = rows // EDGE_TILE
    return pl.pallas_call(
        interface_body,
        out_shape=jax.ShapeDtypeStruct(before.shape, F32),
        in_specs=[IN_HBM, IN_VMEM, IN_VMEM],
        out_specs=IN_HBM,
        scratch_shapes=[pltpu.VMEM((ORDERS, rows, faces), F32), pltpu.SemaphoreType.DMA((tiles,))],
        input_output_aliases={0: 0},
        compiler_params=pltpu.CompilerParams(vmem_limit_bytes=KERNEL_VMEM),
        name="interface_update",
    )(before, edge, ghost)


def on_device(
    moments, courant_azimuth, courant_radial, courant_axial, shear, owner, target, ami_weight
):
    moment = moments[0]
    rows, faces = moment.shape[2], moment.shape[3]
    peers = lax.axis_size("cells")
    regions = lax.axis_size("region")
    cap = max(2, 2 * rows // peers)
    payload, tail = dispatch(owner[0, :, 0], target[0], moment, ami_weight[0], peers, cap)
    received = lax.all_to_all(
        payload.reshape(peers, 1, -1), "cells", split_axis=0, concat_axis=0, tiled=True
    )
    rim = lax.ppermute(tail, "cells", [(i, (i + 1) % peers) for i in range(peers)])
    rim = rim.reshape(ORDERS, -1, rows)
    before, edge = local_update(
        moment, rim[..., None], courant_azimuth[0], courant_radial[0], courant_axial[0], shear[0]
    )
    other = collect(received.reshape(-1, faces), rows, peers, cap)
    ghost = lax.ppermute(other, "region", [(i, regions - 1 - i) for i in range(regions)])
    edge = fetch(edge)
    updated = interface_update(before, edge, ghost)
    return updated[None]


def solution(mesh):
    field = P("region", None, None, "cells")
    cells = P("region", None, None, None, "cells")
    return jax.shard_map(
        on_device,
        mesh=mesh,
        in_specs=(
            cells,
            field,
            field,
            field,
            field,
            P("region", "cells", None),
            P("region", "cells"),
            P("region", "cells", None, None),
        ),
        out_specs=cells,
        check_vma=False,
    )
```

```python
import functools
import math

import jax
import jax.numpy as jnp
from jax import lax
from jax.experimental import pallas as pl
from jax.experimental.pallas import tpu as pltpu
from jax.sharding import PartitionSpec as P


KAGG = 0.005
KBRK = 0.02
ORDERS = 6
F32 = jnp.float32
BF16 = jnp.bfloat16
KERNEL_VMEM = 8 * 1024 * 1024
PAD = 8
GROUP = 8
TILE = 32
EDGE_TILE = 32
FULL_VMEM = 58 * 1024 * 1024
BOUNDS = (0, 2, 5, 8, 11, 14, 16)
AHEAD = 3
RIM_STEP = 3
IN_VMEM = pl.BlockSpec(memory_space=pltpu.VMEM)
IN_HBM = pl.BlockSpec(memory_space=pltpu.HBM)

COS_THIRD = (
    0.44444444535893496,
    0.04115211563399856,
    0.009758495429256357,
    0.0029417445898478234,
    0.0012216398155368902,
    -0.00013418618671007774,
    0.0009423656998505278,
    -0.000598812660480466,
    0.00027219066323123,
)


def two_parts(value):
    high = value.astype(BF16)
    return high, (value - high.astype(F32)).astype(BF16)


def quadrature(moment):
    inv_mass = 1.0 / moment[0]
    n1, n2, n3, n4, n5 = [moment[degree] * inv_mass for degree in range(1, 6)]
    p1 = n2 - n1 * n1
    p2 = n3 - n1 * n2
    p3 = n4 - n1 * n3
    p4 = n5 - n1 * n4
    inv_p1 = 1.0 / p1
    slope = p2 * inv_p1
    a1 = slope - n1
    q2 = p3 - a1 * p2 - p1 * n2
    q3 = p4 - a1 * p3 - p1 * n3
    inv_q2 = 1.0 / q2
    a2 = q3 * inv_q2 - slope
    b2 = q2 * inv_p1
    centre = (n1 + a1 + a2) * (1.0 / 3.0)
    d0 = n1 - centre
    d1 = a1 - centre
    d2 = a2 - centre
    square = (d0 * d0 + d1 * d1 + d2 * d2 + 2.0 * (p1 + b2)) * (1.0 / 6.0)
    inv_h = lax.rsqrt(square)
    h = square * inv_h
    determ = d0 * (d1 * d2 - b2) - p1 * d2
    cosine = jnp.clip(determ * 0.5 * (inv_h * inv_h * inv_h), -1.0, 1.0)
    half = jnp.sqrt(0.5 + 0.5 * cosine)
    w = (0.5 - 0.5 * cosine) / (1.0 + half)
    q = jnp.full_like(w, COS_THIRD[-1])
    for term in COS_THIRD[-2::-1]:
        q = q * w + term
    drop = w * q
    h_cos = h * (1.0 - drop)
    h_sin = h * jnp.sqrt(drop * (2.0 - drop)) * math.sqrt(3.0)
    high = centre + 2.0 * h_cos
    low = centre - h_cos - h_sin
    mid = 3.0 * centre - high - low
    nodes = (low, mid, high)
    weights = []
    for node in nodes:
        u = node - n1
        v = (node - a1) * u - p1
        weights.append(moment[0] / (1.0 + u * u * inv_p1 + v * v * inv_q2))
    return nodes, weights


def sources(moment, shear):
    nodes, weights = quadrature(moment)
    cubes = [node * node * node for node in nodes]
    rate = KBRK * shear
    agg = KAGG * shear
    breaks = [weights[i] * rate * cubes[i] for i in range(3)]
    equal = [weights[i] * agg * (4.0 * cubes[i]) * weights[i] for i in range(3)]
    lost = [2.0 * equal[i] for i in range(3)]
    pairs = []
    for i, j in ((0, 1), (0, 2), (1, 2)):
        summed = nodes[i] + nodes[j]
        pair = weights[i] * weights[j] * (agg * summed * summed * summed)
        lost[i] = lost[i] + pair
        lost[j] = lost[j] + pair
        volume = cubes[i] + cubes[j]
        root = jnp.exp(jnp.log(volume) * (1.0 / 3.0))
        pairs.append((pair, root, volume))
    updated = []
    node_powers = [jnp.ones_like(shear)] * 3
    for degree in range(ORDERS):
        grow = 2.0 ** (degree / 3.0)
        split = 2.0 ** (1.0 - degree / 3.0) - 1.0
        total = moment[degree]
        for i in range(3):
            net = grow * equal[i] - lost[i]
            if degree != 3:
                net = net + split * breaks[i]
            if degree > 0:
                net = net * node_powers[i]
            total = total + net
        for pair, root, volume in pairs:
            factor = (None, root, root * root, volume, volume * root, volume * root * root)[degree]
            total = total + (pair if factor is None else pair * factor)
        updated.append(total)
        node_powers = [power * node for power, node in zip(node_powers, nodes)] if degree else list(nodes)
    return updated


def dispatch_body(
    cap, owner_hbm, target_hbm, moments_hbm, weight_hbm, out, rim,
    moments, weight, source, ids, owner, target, count, index_sem, moment_sem, weight_sem,
):
    layers, rows, faces = moments.shape[1:]
    peers = count.shape[0]
    block = ORDERS * cap + 1
    rotor = lax.axis_index("region") == 0
    layer = jnp.where(rotor, layers - 1, 0)

    def layer_copy(index):
        which = jnp.where(rotor, layers - 1 - index, index)
        return pltpu.make_async_copy(moments_hbm.at[:, which], moments.at[:, which], moment_sem.at[index])

    def weight_copy(step):
        part = pl.ds(BOUNDS[step] * rows // BOUNDS[-1], (BOUNDS[step + 1] - BOUNDS[step]) * rows // BOUNDS[-1])
        return pltpu.make_async_copy(weight_hbm.at[part], weight.at[part], weight_sem.at[step])

    index_copies = (
        pltpu.make_async_copy(owner_hbm, owner, index_sem.at[0]),
        pltpu.make_async_copy(target_hbm, target, index_sem.at[1]),
    )
    layer_copy(0).start()
    for step in range(AHEAD):
        weight_copy(step).start(priority=1)
    for copy in index_copies:
        copy.start()

    out[...] = jnp.zeros_like(out)
    lane = lax.broadcasted_iota(jnp.int32, (1, faces), 1)
    offset = (lax.axis_index("cells") * cap) % faces
    mine = jnp.logical_and(lane >= offset, lane < offset + cap)
    ids[...] = jnp.broadcast_to(jnp.where(mine, -1.0, 0.0), ids.shape)

    @pl.loop(0, peers)
    def _(peer):
        count[peer] = 0

    source[pl.ds(ORDERS * rows, (PAD - ORDERS) * rows)] = jnp.zeros(((PAD - ORDERS) * rows, faces), F32)
    layer_copy(0).wait()
    for degree in range(ORDERS):
        source[pl.ds(degree * rows, rows)] = moments[degree, layer]
    for copy in index_copies:
        copy.wait()
    width = PAD * GROUP
    column = (lax.broadcasted_iota(jnp.int32, (faces, 2 * width), 1) % width) // PAD
    turned = {}

    def turn(step):
        for group in range(BOUNDS[step], BOUNDS[step + 1]):
            first = group * GROUP
            value = jnp.concatenate([source[pl.ds(first + i, PAD, stride=rows)] for i in range(GROUP)], axis=0)
            high = value.astype(BF16).astype(F32)
            turned[group] = jnp.concatenate([high, value - high], axis=0).T

    turn(0)

    def place(first, product):
        product = product.T
        product = product[:width] + product[width:]
        for i in range(GROUP):
            peer = owner[first + i]
            rank = count[peer]
            count[peer] = rank + 1
            out[pl.ds(peer * block + rank * ORDERS, ORDERS), :] = product[PAD * i : PAD * i + ORDERS]
            ids[pl.ds(peer, 1), :] = jnp.where(
                lane == offset + rank, target[first + i].astype(F32), ids[pl.ds(peer, 1), :]
            )

    pending = []
    for step in range(len(BOUNDS) - 1):
        weight_copy(step).wait()
        if step + AHEAD < len(BOUNDS) - 1:
            weight_copy(step + AHEAD).start()
        if step == 0:
            for index in range(1, layers):
                layer_copy(index).start()
        if step + 1 < len(BOUNDS) - 1:
            turn(step + 1)
        products = []
        for group in range(BOUNDS[step], BOUNDS[step + 1]):
            first = group * GROUP
            rhs = jnp.concatenate([jnp.where(column == i, turned[group], 0.0).astype(BF16) for i in range(GROUP)], axis=0)
            parts = [two_parts(weight[first + i]) for i in range(GROUP)]
            product = sum(
                jnp.dot(jnp.concatenate([part[which] for part in parts], axis=1), rhs, preferred_element_type=F32)
                for which in range(2)
            )
            products.append((first, product))
            if pending:
                place(*pending.pop(0))
        if step == RIM_STEP:
            for index in range(1, layers):
                layer_copy(index).wait()
            tail = jnp.zeros((rows, faces), F32)
            wide = lax.broadcasted_iota(jnp.int32, (rows, faces), 1)
            for degree in range(ORDERS):
                for which in range(layers):
                    spot = degree * layers + which
                    tail = jnp.where(wide == spot, pltpu.roll(moments[degree, which], spot + 1, 1), tail)
            rim[...] = tail.T[: ORDERS * layers]
        for item in pending:
            place(*item)
        pending = products
    for item in pending:
        place(*item)

    for peer in range(peers):
        out[pl.ds(peer * block + ORDERS * cap, 1), :] = ids[pl.ds(peer, 1), :]


def dispatch(owner, target, moments, weight, peers, cap):
    layers, rows, faces = moments.shape[1:]
    return pl.pallas_call(
        functools.partial(dispatch_body, cap),
        out_shape=(
            jax.ShapeDtypeStruct((peers * (ORDERS * cap + 1), faces), F32),
            jax.ShapeDtypeStruct((ORDERS * layers, rows), F32),
        ),
        in_specs=[IN_HBM] * 4,
        out_specs=(IN_VMEM, IN_VMEM),
        scratch_shapes=[
            pltpu.VMEM(moments.shape, F32),
            pltpu.VMEM((rows, faces, faces), F32),
            pltpu.VMEM((PAD * rows, faces), F32),
            pltpu.VMEM((peers, faces), F32),
            pltpu.SMEM((rows,), jnp.int32),
            pltpu.SMEM((rows,), jnp.int32),
            pltpu.SMEM((peers,), jnp.int32),
            pltpu.SemaphoreType.DMA((2,)),
            pltpu.SemaphoreType.DMA((layers,)),
            pltpu.SemaphoreType.DMA((len(BOUNDS) - 1,)),
        ],
        compiler_params=pltpu.CompilerParams(vmem_limit_bytes=FULL_VMEM),
        name="dispatch",
    )(owner, target, moments, weight)


def local_body(
    moments_hbm, rim, azim_hbm, radial_hbm, axial_hbm, shear_hbm, out, edge,
    moments, azim, radial, axial, shear, adv, result, sems, load_sems,
):
    layers, rows, faces = moments.shape[1:]
    loads = [
        pltpu.make_async_copy(source, target, load_sems.at[index])
        for index, (source, target) in enumerate(
            ((moments_hbm, moments), (azim_hbm, azim), (radial_hbm, radial), (axial_hbm, axial), (shear_hbm, shear))
        )
    ]
    for load in loads:
        load.start()
    for load in loads:
        load.wait()
    rotor = lax.axis_index("region") == 0
    interface = jnp.where(rotor, layers - 1, 0)
    row = lax.broadcasted_iota(jnp.int32, (rows, faces), 0)
    lane = lax.broadcasted_iota(jnp.int32, (rows, faces), 1)

    def advect(layer, target):
        ca = azim[layer]
        cr = radial[layer]
        cz = axial[layer]
        outward = jnp.maximum(cr, 0.0)
        inward = outward - cr
        upward = jnp.maximum(cz, 0.0)
        downward = upward - cz
        keep = 1.0 - ca - (outward + inward) - (upward + downward)
        outward = jnp.where(layer > 0, outward, 0.0)
        inward = jnp.where(layer < layers - 1, inward, 0.0)
        upward = jnp.where(row > 0, upward, 0.0)
        downward = jnp.where(row < rows - 1, downward, 0.0)
        below = jnp.maximum(layer - 1, 0)
        beyond = jnp.minimum(layer + 1, layers - 1)
        for degree in range(ORDERS):
            m = moments[degree, layer]
            prev = jnp.where(lane == 0, rim[degree, layer], pltpu.roll(m, 1, 1))
            target[degree] = (
                keep * m
                + ca * prev
                + outward * moments[degree, below]
                + inward * moments[degree, beyond]
                + upward * pltpu.roll(m, 1, 0)
                + downward * pltpu.roll(m, rows - 1, 0)
            )

    def store(index, layer):
        return pltpu.make_async_copy(result.at[index], out.at[:, layer], sems.at[index])

    @pl.loop(0, layers - 1)
    def _(index):
        layer = jnp.where(rotor, index, index + 1)
        advect(layer, adv)

        @pl.loop(0, rows // TILE)
        def _(step):
            part = pl.ds(pl.multiple_of(step * TILE, TILE), TILE)
            updated = sources([adv[degree, part] for degree in range(ORDERS)], shear[layer, part])
            for degree in range(ORDERS):
                result[index, degree, part] = updated[degree]

        store(index, layer).start()

    advect(interface, edge)
    outward = jnp.maximum(radial[interface], 0.0)
    edge[ORDERS] = jnp.where(rotor, outward - radial[interface], outward)
    edge[ORDERS + 1] = shear[interface]

    @pl.loop(0, layers - 1)
    def _(index):
        store(index, jnp.where(rotor, index, index + 1)).wait()


def local_update(moments, rim, azim, radial, axial, shear):
    layers, rows, faces = moments.shape[1:]
    return pl.pallas_call(
        local_body,
        out_shape=(
            jax.ShapeDtypeStruct(moments.shape, F32),
            jax.ShapeDtypeStruct((ORDERS + 2, rows, faces), F32),
        ),
        in_specs=[IN_HBM, IN_VMEM] + [IN_HBM] * 4,
        out_specs=(IN_HBM, IN_VMEM),
        scratch_shapes=[pltpu.VMEM(moments.shape, F32)]
        + [pltpu.VMEM(azim.shape, F32)] * 4
        + [
            pltpu.VMEM((ORDERS, rows, faces), F32),
            pltpu.VMEM((layers - 1, ORDERS, rows, faces), F32),
            pltpu.SemaphoreType.DMA((layers - 1,)),
            pltpu.SemaphoreType.DMA((5,)),
        ],
        compiler_params=pltpu.CompilerParams(vmem_limit_bytes=FULL_VMEM),
        name="local_update",
    )(moments, rim, azim, radial, axial, shear)


def collect_body(peers, cap, received, out, gathered):
    rows, faces = out.shape[1], out.shape[2]
    block = ORDERS * cap + 1
    per_row = faces // cap
    row_id = lax.broadcasted_iota(jnp.int32, (rows, faces), 0).astype(F32)
    hits = []
    for first in range(0, peers, per_row):
        ids = jnp.zeros((1, faces), F32)
        for peer in range(first, min(peers, first + per_row)):
            ids = ids + received[pl.ds(peer * block + ORDERS * cap, 1), :]
        hits.append((row_id == ids).astype(BF16))
    hits = jnp.concatenate(hits, axis=1)
    for degree in range(ORDERS):
        for peer in range(peers):
            gathered[pl.ds(peer * cap, cap), :] = received[pl.ds(peer * block + degree, cap, stride=ORDERS), :]
        high, low = two_parts(gathered[...])
        out[degree] = jnp.dot(hits, high, preferred_element_type=F32) + jnp.dot(
            hits, low, preferred_element_type=F32
        )


def collect(received, rows, peers, cap):
    faces = received.shape[1]
    return pl.pallas_call(
        functools.partial(collect_body, peers, cap),
        out_shape=jax.ShapeDtypeStruct((ORDERS, rows, faces), F32),
        in_specs=[IN_VMEM],
        out_specs=IN_VMEM,
        scratch_shapes=[pltpu.VMEM((peers * cap, faces), F32)],
        compiler_params=pltpu.CompilerParams(vmem_limit_bytes=KERNEL_VMEM),
        name="collect",
    )(received)


def fetch_body(source, out, sem):
    copy = pltpu.make_async_copy(source, out, sem)
    copy.start()
    copy.wait()


def fetch(edge):
    return pl.pallas_call(
        fetch_body,
        out_shape=jax.ShapeDtypeStruct(edge.shape, F32),
        in_specs=[IN_HBM],
        out_specs=IN_VMEM,
        scratch_shapes=[pltpu.SemaphoreType.DMA],
        compiler_params=pltpu.CompilerParams(vmem_limit_bytes=KERNEL_VMEM),
        name="fetch",
    )(edge)


def interface_body(before, edge, ghost, out, result, sems):
    rows = ghost.shape[1]
    tiles = sems.shape[0]
    tile = rows // tiles
    layer = jnp.where(lax.axis_index("region") == 0, out.shape[1] - 1, 0)

    def store(step):
        part = pl.ds(step * tile, tile)
        return pltpu.make_async_copy(result.at[:, part], out.at[:, layer, part], sems.at[step])

    for step in range(tiles):
        part = pl.ds(step * tile, tile)
        share = edge[ORDERS, part]
        moment = [edge[degree, part] + share * ghost[degree, part] for degree in range(ORDERS)]
        updated = sources(moment, edge[ORDERS + 1, part])
        for degree in range(ORDERS):
            result[degree, part] = updated[degree]
        store(step).start()
    for step in range(tiles):
        store(step).wait()


def interface_update(before, edge, ghost):
    rows, faces = ghost.shape[1:]
    tiles = rows // EDGE_TILE
    return pl.pallas_call(
        interface_body,
        out_shape=jax.ShapeDtypeStruct(before.shape, F32),
        in_specs=[IN_HBM, IN_VMEM, IN_VMEM],
        out_specs=IN_HBM,
        scratch_shapes=[pltpu.VMEM((ORDERS, rows, faces), F32), pltpu.SemaphoreType.DMA((tiles,))],
        input_output_aliases={0: 0},
        compiler_params=pltpu.CompilerParams(vmem_limit_bytes=KERNEL_VMEM),
        name="interface_update",
    )(before, edge, ghost)


def on_device(
    moments, courant_azimuth, courant_radial, courant_axial, shear, owner, target, ami_weight
):
    moment = moments[0]
    rows, faces = moment.shape[2], moment.shape[3]
    peers = lax.axis_size("cells")
    regions = lax.axis_size("region")
    cap = max(2, 2 * rows // peers)
    payload, tail = dispatch(owner[0, :, 0], target[0], moment, ami_weight[0], peers, cap)
    received = lax.all_to_all(
        payload.reshape(peers, 1, -1), "cells", split_axis=0, concat_axis=0, tiled=True
    )
    rim = lax.ppermute(tail, "cells", [(i, (i + 1) % peers) for i in range(peers)])
    rim = rim.reshape(ORDERS, -1, rows)
    before, edge = local_update(
        moment, rim[..., None], courant_azimuth[0], courant_radial[0], courant_axial[0], shear[0]
    )
    other = collect(received.reshape(-1, faces), rows, peers, cap)
    ghost = lax.ppermute(other, "region", [(i, regions - 1 - i) for i in range(regions)])
    edge = fetch(edge)
    updated = interface_update(before, edge, ghost)
    return updated[None]


def solution(mesh):
    field = P("region", None, None, "cells")
    cells = P("region", None, None, None, "cells")
    return jax.shard_map(
        on_device,
        mesh=mesh,
        in_specs=(
            cells,
            field,
            field,
            field,
            field,
            P("region", "cells", None),
            P("region", "cells"),
            P("region", "cells", None, None),
        ),
        out_specs=cells,
        check_vma=False,
    )
```
